128 devices in a mesh: gx: 4 (over x_lo, core), gy: 4 (over y), gz: 8 (over x_hi, z).
Axes of the slice: x: 4 (x_hi: 2, x_lo: 2; x = x_hi * 2 + x_lo), y: 4, z: 4, core: 2. Of those that a mesh axis runs over, the one named last changes fastest.
Arguments:
- inv_factor: bfloat16 [4, 4, 8, 1536, 1536], P('gx', 'gy', 'gz'), as said below
- coupling: bfloat16 [4, 4, 8, 1536, 1536], P('gx', 'gy', 'gz'), may hold values from -0.15625 to 0.15625
- stiff_gg: bfloat16 [4, 4, 8, 1536, 1536], P('gx', 'gy', 'gz'), as said below
- block_order: int32 [4, 4, 8, 12], P('gx', 'gy', 'gz'), may hold values from 0 to 11, each once within a row
Outputs:
- assembled: float32 [4, 4, 8, 1536, 1536], P('gx', 'gy', 'gz')
The draws below stay inside these ranges and needn't reach their ends.
Inputs may be any that keep to these rules, and one draw needn't show every extreme that they name: `block_order`: each subdomain's row is a permutation of 0 to 11. `stiff_gg`: each subdomain's block is symmetric. `inv_factor`: each subdomain's block is lower triangular with a positive diagonal.
All inputs are finite; a program needn't handle non-finite values.
Results may differ from the reference program's by a relative error of at most 0.0016.
Values sent between devices are 32-bit elements; how exact they have to be, the bound alone decides.
A program may use at most 128 MiB of HBM per device.

```python
import math
import jax
import jax.numpy as jnp
import numpy as np
from jax import lax

NI = 1536
BLK = 128
NBLK = 12
NG = 1536
SUB_X = 4
SUB_Y = 4
SUB_Z = 8


def draw_inv_factor(key, part):
    shape = (SUB_X, SUB_Y, SUB_Z, NI, NI)
    first_key, second_key = jax.random.split(jax.random.fold_in(key, 11))
    entries = jax.random.normal(first_key, shape, jnp.float32)
    lower = jnp.tril(entries, -1) / math.sqrt(NI)
    diagonal = jax.random.uniform(second_key, shape[:-1], jnp.float32, 0.5, 1.5)
    return (lower + diagonal[..., None] * jnp.eye(NI, dtype=jnp.float32)).astype(jnp.bfloat16)


def draw_stiff_gg(key, part):
    shape = (SUB_X, SUB_Y, SUB_Z, NG, NG)
    first_key, second_key = jax.random.split(jax.random.fold_in(key, 23))
    base = jax.random.normal(first_key, shape, jnp.float32)
    symmetric = (base + jnp.swapaxes(base, -1, -2)) / math.sqrt(2.0 * NG)
    diagonal = jax.random.uniform(second_key, shape[:-1], jnp.float32, 2.0, 4.0)
    return (symmetric + diagonal[..., None] * jnp.eye(NG, dtype=jnp.float32)).astype(jnp.bfloat16)


def block_levels(rng, shape, shards, smallest, top_value):
    gain, own = 1.0, jax.random.fold_in(rng, 6)
    for position, parts in shards:
        steps = jnp.exp(jax.random.uniform(jax.random.fold_in(own, position), (parts,), jnp.float32, smallest / len(shards), top_value / len(shards)))
        gain = gain * jnp.repeat(steps, shape[position] // parts).reshape([-1 if axis == position else 1 for axis in range(len(shape))])
    return gain


def bell_draw(rng, shape, scale, limit, cuts=(), kind=jnp.bfloat16):
    values = jax.random.normal(rng, shape, jnp.float32) * scale
    if len(cuts) > 0:
        values = block_levels(rng, shape, cuts, -0.22, 0.18) * values
    return jnp.clip(values, min=-limit, max=limit).astype(kind)


def setup_inputs(seed: int = 0) -> dict:
    keys = jax.random.split(jax.random.key(seed), 5)
    return {
        "inv_factor": draw_inv_factor(jax.random.fold_in(keys[4], 71), 0),
        "coupling": bell_draw(keys[1], (SUB_X, SUB_Y, SUB_Z, NI, NG), NI ** -0.5, 0.15625, ((0, 4), (1, 4), (2, 8))),
        "stiff_gg": draw_stiff_gg(jax.random.fold_in(keys[4], 71), 0),
        "block_order": jax.vmap(lambda own: jax.random.permutation(own, NBLK))(jax.random.split(keys[3], SUB_X * SUB_Y * SUB_Z)).reshape((SUB_X, SUB_Y, SUB_Z, NBLK)).astype(jnp.int32),
    }


west_blocks = (0,)
east_blocks = (1,)
south_blocks = (2, 8, 10)
north_blocks = (3, 9, 11)
bottom_blocks = (4, 5, 8, 9)
top_blocks = (6, 7, 10, 11)


def local_tile(operands):
    inverse, coupled, stiffness = operands
    weighted = jnp.dot(inverse, coupled, preferred_element_type=jnp.float32).astype(jnp.bfloat16)
    product = jnp.dot(weighted.T, weighted, preferred_element_type=jnp.float32)
    return stiffness.astype(jnp.float32) - product


def reorder(matrix, ranking):
    return matrix[ranking][:, ranking]


def shifted(values, axis, direction):
    extent = values.shape[axis]
    zeros_edge = jnp.zeros_like(lax.slice_in_dim(values, 0, 1, axis=axis))
    if direction > 0:
        return jnp.concatenate([zeros_edge, lax.slice_in_dim(values, 0, extent - 1, axis=axis)], axis)
    return jnp.concatenate([lax.slice_in_dim(values, 1, extent, axis=axis), zeros_edge], axis)


def section_sum(grid, axis, lower_list, upper_list):
    lower_idx = np.array(lower_list, dtype=np.int32)
    upper_idx = np.array(upper_list, dtype=np.int32)
    lower_piece = grid[:, :, :, lower_idx][:, :, :, :, lower_idx]
    upper_piece = grid[:, :, :, upper_idx][:, :, :, :, upper_idx]
    from_lower = shifted(upper_piece, axis, 1)
    from_upper = shifted(lower_piece, axis, -1)
    grid = grid.at[:, :, :, lower_idx[:, None], lower_idx[None, :]].add(from_lower)
    grid = grid.at[:, :, :, upper_idx[:, None], upper_idx[None, :]].add(from_upper)
    return grid


def reference(inv_factor, coupling, stiff_gg, block_order):
    total = SUB_X * SUB_Y * SUB_Z
    tiles = lax.map(local_tile, (inv_factor.reshape(total, NI, NI), coupling.reshape(total, NI, NG), stiff_gg.reshape(total, NG, NG)))
    blocked = tiles.reshape(total, NBLK, BLK, NBLK, BLK).transpose(0, 1, 3, 2, 4)
    ranks = block_order.reshape(total, NBLK).astype(jnp.int32)
    canonical = jax.vmap(reorder)(blocked, ranks)
    grid = canonical.reshape(SUB_X, SUB_Y, SUB_Z, NBLK, NBLK, BLK, BLK)
    grid = section_sum(grid, 0, west_blocks, east_blocks)
    grid = section_sum(grid, 1, south_blocks, north_blocks)
    grid = section_sum(grid, 2, bottom_blocks, top_blocks)
    inverse_rank = jnp.argsort(ranks, axis=1).astype(jnp.int32)
    own = jax.vmap(reorder)(grid.reshape(total, NBLK, NBLK, BLK, BLK), inverse_rank)
    return own.transpose(0, 1, 3, 2, 4).reshape(SUB_X, SUB_Y, SUB_Z, NG, NG)
```

```python
import jax
import jax.numpy as jnp
from jax import lax
from jax.experimental import pallas as pl
from jax.experimental.pallas import tpu as pltpu
from jax.sharding import PartitionSpec as P

BLK = 128
NBLK = 12
TILE = 2 * BLK
NTILE = NBLK // 2
MESH = pl.DeviceIdType.MESH
F32 = jnp.float32
BF16 = jnp.bfloat16

STORED = (8, 9, 10, 11, 4, 5, 6, 7, 2, 3, 0, 1)
PLACE = {block: place for place, block in enumerate(STORED)}

SECTIONS = {
    "x": ("gx", (0,), (1,)),
    "y": ("gy", (8, 10, 2), (9, 11, 3)),
    "z": ("gz", (8, 9, 4, 5), (10, 11, 6, 7)),
}


def pairs_of(name):
    count = len(SECTIONS[name][1])
    return [(i, j) for i in range(count) for j in range(i + 1)]


def schur_kernel(order, inv_h, cpl_h, stf_h, tile, *scratch):
    cpl = scratch[:NTILE]
    inv, stf, w, wt = scratch[NTILE : NTILE + 4]
    load_sem = scratch[NTILE + 4]
    got = dict(zip("xyz", scratch[NTILE + 5 : NTILE + 8]))
    send_sem = dict(zip("xyz", scratch[NTILE + 8 : NTILE + 11]))
    recv_sem = dict(zip("xyz", scratch[NTILE + 11 : NTILE + 14]))

    def span(i, size=TILE):
        return slice(i * size, (i + 1) * size)

    loads = []
    for i in range(NTILE):
        area = (span(i), slice(0, (i + 1) * TILE))
        group = [pltpu.make_async_copy(inv_h.at[area], inv.at[area], load_sem.at[i, NBLK])]
        for s in range(NBLK):
            group.append(
                pltpu.make_async_copy(
                    cpl_h.at[span(i), span(s, BLK)], cpl[i].at[s], load_sem.at[i, s]
                )
            )
        loads.append(group)
    load_stf = [
        pltpu.make_async_copy(stf_h.at[:, :, span(s, BLK)], stf.at[s], load_sem.at[NTILE, s])
        for s in range(NBLK)
    ]
    for group in loads + [load_stf]:
        for load in group:
            load.start()

    spot = {name: lax.axis_index(SECTIONS[name][0]) for name in "xyz"}
    size = {name: lax.axis_size(SECTIONS[name][0]) for name in "xyz"}
    lower = {name: spot[name] > 0 for name in "xyz"}
    upper = {name: spot[name] < size[name] - 1 for name in "xyz"}

    barrier = pltpu.get_barrier_semaphore()
    for name in "xyz":
        axis = SECTIONS[name][0]
        for there, step in ((lower[name], -1), (upper[name], 1)):

            @pl.when(there)
            def _(axis=axis, name=name, step=step):
                pl.semaphore_signal(
                    barrier, inc=1, device_id={axis: spot[name] + step}, device_id_type=MESH
                )

    def greet():
        peers = sum(
            there[name].astype(jnp.int32) for there in (lower, upper) for name in "xyz"
        )
        pl.semaphore_wait(barrier, peers)

    def block(a, b):
        return tile.at[PLACE[a], PLACE[b]]

    def copy(name, side, number):
        axis, *lists = SECTIONS[name]
        i, j = pairs_of(name)[number]
        return pltpu.make_async_remote_copy(
            src_ref=block(lists[side][i], lists[side][j]),
            dst_ref=got[name].at[side, number],
            send_sem=send_sem[name].at[side, number],
            recv_sem=recv_sem[name].at[side, number],
            device_id={axis: spot[name] + (1 if side else -1)},
            device_id_type=MESH,
        )

    def send(name, side, numbers):
        @pl.when(upper[name] if side else lower[name])
        def _():
            for number in numbers:
                copy(name, side, number).start()

    def absorb(name, side, numbers):
        lists = SECTIONS[name][1:]

        @pl.when(upper[name] if side else lower[name])
        def _():
            for number in numbers:
                i, j = pairs_of(name)[number]
                a, b = lists[side][i], lists[side][j]
                copy(name, side, number).wait_send()
                copy(name, 1 - side, number).wait_recv()
                value = got[name][1 - side, number]
                block(a, b)[...] += value
                if i != j:
                    block(b, a)[...] += value.T

    def place(stored):
        return order[0, 0, 0, STORED[stored]]

    def columns(i, tiles):
        return jnp.concatenate(
            [cpl[i][place(s)] for t in tiles for s in (2 * t, 2 * t + 1)], axis=1
        )

    def weigh(i, tiles):
        depth = (i + 1) * TILE
        right = jnp.concatenate([columns(k, tiles) for k in range(i + 1)], axis=0)
        part = jnp.dot(inv[span(i), :depth], right, preferred_element_type=F32).astype(BF16)
        cols = slice(tiles[0] * TILE, (tiles[-1] + 1) * TILE)
        w[span(i), cols] = part
        wt[cols, span(i)] = part.T

    def product(t, u):
        both = jnp.dot(wt[span(t), :], w[:, span(u)], preferred_element_type=F32)
        for p in range(2):
            for q in range(2):
                r, c = 2 * t + p, 2 * u + q
                own = stf[place(c), place(r)].astype(F32)
                value = own - both[span(p, BLK), span(q, BLK)]
                tile[r, c] = value
                if t != u:
                    tile[c, r] = value.T

    for i in range(NTILE):
        for load in loads[i]:
            load.wait()
        weigh(i, (0, 1))
    for load in load_stf:
        load.wait()
    number_of = {name: {pair: n for n, pair in enumerate(pairs_of(name))} for name in "xyz"}
    zn, yn = number_of["z"], number_of["y"]

    product(0, 0)
    greet()
    send("y", 0, [yn[0, 0]])
    send("y", 1, [yn[0, 0]])
    send("z", 0, [zn[1, 0]])
    product(1, 1)
    send("y", 0, [yn[1, 1]])
    send("y", 1, [yn[1, 1]])
    send("z", 1, [zn[1, 0]])
    for i in range(NTILE):
        weigh(i, (2,))
    product(2, 0)
    send("z", 0, [zn[2, 0], zn[2, 1], zn[3, 0], zn[3, 1]])
    for i in range(NTILE):
        weigh(i, (3,))
    product(3, 1)
    send("z", 1, [zn[2, 0], zn[2, 1], zn[3, 0], zn[3, 1]])
    product(2, 2)
    send("z", 0, [zn[2, 2], zn[3, 2], zn[3, 3]])
    product(3, 3)
    send("z", 1, [zn[2, 2], zn[3, 2], zn[3, 3]])
    product(1, 0)
    send("y", 0, [yn[1, 0]])
    send("y", 1, [yn[1, 0]])
    for i in range(NTILE):
        weigh(i, (4,))
    product(4, 0)
    product(4, 1)
    product(4, 4)
    send("y", 0, [yn[2, 0], yn[2, 1], yn[2, 2]])
    send("y", 1, [yn[2, 0], yn[2, 1], yn[2, 2]])
    for side in (0, 1):
        absorb("y", side, [yn[0, 0], yn[1, 1]])
    for side in (0, 1):
        send("z", side, [zn[0, 0], zn[1, 1]])
    for i in range(NTILE):
        weigh(i, (5,))
    product(5, 5)
    send("x", 0, [0])
    send("x", 1, [0])
    for t, u in ((2, 1), (3, 0), (3, 2), (4, 2), (4, 3), (5, 0), (5, 1), (5, 2), (5, 3), (5, 4)):
        product(t, u)
    for side in (0, 1):
        absorb("y", side, [yn[1, 0], yn[2, 0], yn[2, 1], yn[2, 2]])
    for side in (0, 1):
        absorb("x", side, [0])
    late = [zn[0, 0], zn[1, 1]]
    soon = [n for n in range(len(pairs_of("z"))) if n not in late]
    for side in (0, 1):
        absorb("z", side, soon)
    for side in (0, 1):
        absorb("z", side, late)


def place_kernel(order, tile, out, sem):
    def moves(do):
        for r in range(NBLK):
            row = pl.multiple_of(order[0, 0, 0, STORED[r]] * BLK, BLK)
            for c in range(NBLK):
                col = pl.multiple_of(order[0, 0, 0, STORED[c]] * BLK, BLK)
                do(
                    pltpu.make_async_copy(
                        tile.at[r, c], out.at[pl.ds(row, BLK), pl.ds(col, BLK)], sem.at[r, c]
                    )
                )

    moves(lambda move: move.start())
    moves(lambda move: move.wait())


def shards(inv_factor, coupling, stiff_gg, block_order):
    full = NBLK * BLK
    hbm = pl.BlockSpec(memory_space=pltpu.HBM)
    smem = pl.BlockSpec(memory_space=pltpu.SMEM)
    vmem = pl.BlockSpec(memory_space=pltpu.VMEM)
    counts = {name: len(pairs_of(name)) for name in "xyz"}
    tile = pl.pallas_call(
        schur_kernel,
        out_shape=pltpu.VMEM((NBLK, NBLK, BLK, BLK), F32),
        in_specs=[smem, hbm, hbm, hbm],
        out_specs=vmem,
        scratch_shapes=[pltpu.VMEM((NBLK, TILE, BLK), BF16) for _ in range(NTILE)]
        + [pltpu.VMEM((full, full), BF16)]
        + [pltpu.VMEM((NBLK, NBLK, BLK, BLK), BF16)]
        + [pltpu.VMEM((full, full), BF16) for _ in range(2)]
        + [pltpu.SemaphoreType.DMA((NTILE + 1, NBLK + 1))]
        + [pltpu.VMEM((2, counts[name], BLK, BLK), F32) for name in "xyz"]
        + [pltpu.SemaphoreType.DMA((2, counts[name])) for name in "xyz"]
        + [pltpu.SemaphoreType.DMA((2, counts[name])) for name in "xyz"],
        compiler_params=pltpu.CompilerParams(
            collective_id=0, has_side_effects=True, vmem_limit_bytes=44 << 20
        ),
        name="schur",
    )(
        block_order,
        inv_factor.reshape(full, full),
        coupling.reshape(full, full),
        stiff_gg.reshape(NBLK, BLK, full),
    )
    own = pl.pallas_call(
        place_kernel,
        out_shape=jax.ShapeDtypeStruct((full, full), F32),
        in_specs=[smem, vmem],
        out_specs=hbm,
        scratch_shapes=[pltpu.SemaphoreType.DMA((NBLK, NBLK))],
        compiler_params=pltpu.CompilerParams(vmem_limit_bytes=20 << 20),
        name="place",
    )(block_order, tile)
    return own.reshape(1, 1, 1, full, full)


def solution(mesh):
    return jax.shard_map(
        shards,
        mesh=mesh,
        in_specs=(
            P("gx", "gy", "gz", None, None),
            P("gx", "gy", "gz", None, None),
            P("gx", "gy", "gz", None, None),
            P("gx", "gy", "gz", None),
        ),
        out_specs=P("gx", "gy", "gz", None, None),
        check_vma=False,
    )
```

```python
import jax
import jax.numpy as jnp
from jax import lax
from jax.experimental import pallas as pl
from jax.experimental.pallas import tpu as pltpu
from jax.sharding import PartitionSpec as P

BLK = 128
NBLK = 12
TILE = 2 * BLK
NTILE = NBLK // 2
FOLD = BLK + 8
MESH = pl.DeviceIdType.MESH
F32 = jnp.float32
BF16 = jnp.bfloat16

STORED = (8, 9, 10, 11, 4, 6, 5, 7, 2, 3, 0, 1)
PLACE = {block: place for place, block in enumerate(STORED)}

SECTIONS = {
    "x": ("gx", (0,), (1,)),
    "y": ("gy", (8, 10, 2), (9, 11, 3)),
    "z": ("gz", (8, 9, 4, 5), (10, 11, 6, 7)),
}
BLOCKS = {
    "x": (((0, 0),),),
    "y": (((1, 0), (2, 0), (2, 1), (2, 2)),),
    "z": (((1, 0), (2, 0), (2, 1)), ((3, 0), (3, 1), (3, 2))),
}
FOLDS = {"x": (), "y": ((0, 1),), "z": ((2, 3), (0, 1))}
NUMBER = {
    name: {pair: n for n, pair in enumerate(pair for group in groups for pair in group)}
    for name, groups in BLOCKS.items()
}
START = {
    name: [sum(len(group) for group in groups[:g]) for g in range(len(groups))]
    for name, groups in BLOCKS.items()
}


def schur_kernel(order_h, inv_h, cpl_h, stf_h, tile, *scratch):
    scratch = list(scratch)
    cpl = [scratch.pop(0) for _ in range(NTILE)]
    inv, stf, w, wt, order, load_sem = (scratch.pop(0) for _ in range(6))
    got = {name: scratch.pop(0) for name in "xyz"}
    send_sem = {name: scratch.pop(0) for name in "xyz"}
    recv_sem = {name: scratch.pop(0) for name in "xyz"}
    folded = {name: scratch.pop(0) for name in "yz"}
    got_fold = {name: scratch.pop(0) for name in "yz"}
    fold_send_sem = {name: scratch.pop(0) for name in "yz"}
    fold_recv_sem = {name: scratch.pop(0) for name in "yz"}

    def span(i, size=TILE):
        return slice(i * size, (i + 1) * size)

    load_order = pltpu.make_async_copy(order_h, order, load_sem.at[2 * NTILE + 1])
    load_order.start()
    load_inv = []
    for i in range(NTILE):
        area = (span(i), slice(0, (i + 1) * TILE))
        load_inv.append(pltpu.make_async_copy(inv_h.at[area], inv.at[area], load_sem.at[i]))
        load_inv[i].start()
        for s in range(NBLK):
            pltpu.make_async_copy(
                cpl_h.at[span(i), span(s, BLK)], cpl[i].at[s], load_sem.at[NTILE + i]
            ).start()
    for r in range(NBLK):
        for c in range(r + 1):
            pltpu.make_async_copy(
                stf_h.at[span(r, BLK), span(c, BLK)],
                stf.at[r * (r + 1) // 2 + c],
                load_sem.at[2 * NTILE],
            ).start()

    spot = {name: lax.axis_index(SECTIONS[name][0]) for name in "xyz"}
    size = {name: lax.axis_size(SECTIONS[name][0]) for name in "xyz"}
    there = {
        name: (spot[name] > 0, spot[name] < size[name] - 1) for name in "xyz"
    }

    barrier = pltpu.get_barrier_semaphore()
    for name in "xyz":
        for side in (0, 1):

            @pl.when(there[name][side])
            def _(name=name, side=side):
                pl.semaphore_signal(
                    barrier,
                    inc=1,
                    device_id={SECTIONS[name][0]: spot[name] + 2 * side - 1},
                    device_id_type=MESH,
                )

    def greet():
        peers = sum(there[name][side].astype(jnp.int32) for side in (0, 1) for name in "xyz")
        pl.semaphore_wait(barrier, peers)

    def block(a, b):
        return tile.at[PLACE[a], PLACE[b]]

    def remote(name, side, source, target, leave, arrive):
        return pltpu.make_async_remote_copy(
            src_ref=source,
            dst_ref=target,
            send_sem=leave,
            recv_sem=arrive,
            device_id={SECTIONS[name][0]: spot[name] + 2 * side - 1},
            device_id_type=MESH,
        )

    def group_of(name, pair):
        return [pair in group for group in BLOCKS[name]].index(True)

    def send(name, pairs):
        for side in (0, 1):
            send_side(name, side, pairs)

    def send_side(name, side, pairs):
        listed = SECTIONS[name][1 + side]

        @pl.when(there[name][side])
        def _():
            for pair in pairs:
                remote(
                    name,
                    side,
                    block(listed[pair[0]], listed[pair[1]]),
                    got[name].at[side, NUMBER[name][pair]],
                    send_sem[name].at[side],
                    recv_sem[name].at[side, group_of(name, pair)],
                ).start()

    def wait_sent(name):
        for side in (0, 1):

            @pl.when(there[name][side])
            def _(side=side):
                whole = got[name].at[side]
                remote(
                    name, side, whole, whole, send_sem[name].at[side], recv_sem[name].at[side, 0]
                ).wait_send()

    def absorb(name, group):
        pairs = BLOCKS[name][group]
        first = START[name][group]
        for side in (0, 1):
            listed = SECTIONS[name][1 + side]

            @pl.when(there[name][side])
            def _(side=side, listed=listed):
                area = got[name].at[1 - side, slice(first, first + len(pairs))]
                remote(
                    name,
                    side,
                    area,
                    area,
                    send_sem[name].at[side],
                    recv_sem[name].at[1 - side, group],
                ).wait_recv()
                for n, (i, j) in enumerate(pairs):
                    a, b = listed[i], listed[j]
                    value = got[name][1 - side, first + n]
                    block(a, b)[...] += value
                    if i != j:
                        block(b, a)[...] += value.T

    rows = lax.broadcasted_iota(jnp.int32, (BLK, BLK), 0)
    cols = lax.broadcasted_iota(jnp.int32, (BLK, BLK), 1)

    def fold(name, number):
        i, j = FOLDS[name][number]
        for side in (0, 1):
            listed = SECTIONS[name][1 + side]

            @pl.when(there[name][side])
            def _(side=side, listed=listed):
                one = block(listed[i], listed[i])[...]
                two = block(listed[j], listed[j])[...]
                where = folded[name].at[side, number]
                where[:BLK] = jnp.where(rows >= cols, one, two)
                line = jnp.sum(jnp.where(rows == cols, two, 0.0), axis=0, keepdims=True)
                where[BLK:] = jnp.broadcast_to(line, (FOLD - BLK, BLK))
                remote(
                    name,
                    side,
                    where,
                    got_fold[name].at[side, number],
                    fold_send_sem[name].at[side],
                    fold_recv_sem[name].at[side, number],
                ).start()

    def unfold(name, number):
        i, j = FOLDS[name][number]
        for side in (0, 1):
            listed = SECTIONS[name][1 + side]

            @pl.when(there[name][side])
            def _(side=side, listed=listed):
                area = got_fold[name].at[1 - side, number]
                remote(
                    name,
                    side,
                    area,
                    area,
                    fold_send_sem[name].at[side],
                    fold_recv_sem[name].at[1 - side, number],
                ).wait_recv()
                body = area[:BLK]
                line = area[BLK : BLK + 1]
                flip = body.T
                block(listed[i], listed[i])[...] += jnp.where(rows >= cols, body, flip)
                two = jnp.where(rows == cols, jnp.broadcast_to(line, (BLK, BLK)), flip)
                block(listed[j], listed[j])[...] += jnp.where(rows < cols, body, two)

    def wait_folds(name):
        for side in (0, 1):

            @pl.when(there[name][side])
            def _(side=side):
                whole = folded[name].at[side]
                remote(
                    name,
                    side,
                    whole,
                    whole,
                    fold_send_sem[name].at[side],
                    fold_recv_sem[name].at[side, 0],
                ).wait_send()

    def columns(i, tiles):
        return jnp.concatenate(
            [cpl[i][order[0, 0, 0, STORED[s]]] for t in tiles for s in (2 * t, 2 * t + 1)], axis=1
        )

    def weigh(i, tiles):
        depth = (i + 1) * TILE
        right = jnp.concatenate([columns(k, tiles) for k in range(i + 1)], axis=0)
        part = jnp.dot(inv[span(i), :depth], right, preferred_element_type=F32).astype(BF16)
        across = slice(tiles[0] * TILE, (tiles[-1] + 1) * TILE)
        w[span(i), across] = part
        wt[across, span(i)] = part.T

    def stiffness(r, c):
        row, col = order[0, 0, 0, STORED[r]], order[0, 0, 0, STORED[c]]
        high, low = jnp.maximum(row, col), jnp.minimum(row, col)
        held = stf[lax.shift_right_logical(high * (high + 1), 1) + low].astype(F32)
        return held if r == c else jnp.where(row > col, held, held.T)

    def product(t, u):
        both = jnp.dot(wt[span(t), :], w[:, span(u)], preferred_element_type=F32)
        for p in range(2):
            for q in range(2):
                r, c = 2 * t + p, 2 * u + q
                if r < c:
                    continue
                value = stiffness(r, c) - both[span(p, BLK), span(q, BLK)]
                tile[r, c] = value
                if r != c:
                    tile[c, r] = value.T

    load_order.wait()
    for i in range(NTILE):
        load_inv[i].wait()
        pltpu.make_async_copy(cpl[i], cpl[i], load_sem.at[NTILE + i]).wait()
        weigh(i, (0, 1))
    pltpu.make_async_copy(stf, stf, load_sem.at[2 * NTILE]).wait()

    product(0, 0)
    greet()
    send_side("z", 0, [(1, 0)])
    product(1, 1)
    send_side("z", 1, [(1, 0)])
    fold("y", 0)
    product(1, 0)
    send("y", [(1, 0)])
    for i in range(NTILE):
        weigh(i, (2,))
    product(2, 0)
    send_side("z", 0, [(2, 0), (2, 1)])
    product(2, 1)
    send_side("z", 1, [(2, 0), (2, 1)])
    for i in range(NTILE):
        weigh(i, (3,))
    product(3, 0)
    send_side("z", 0, [(3, 0), (3, 1)])
    product(3, 1)
    send_side("z", 1, [(3, 0), (3, 1)])
    product(3, 2)
    send("z", [(3, 2)])
    product(2, 2)
    product(3, 3)
    fold("z", 0)
    for i in range(NTILE):
        weigh(i, (4,))
    product(4, 0)
    product(4, 1)
    product(4, 4)
    send("y", [(2, 0), (2, 1), (2, 2)])
    unfold("y", 0)
    fold("z", 1)
    for i in range(NTILE):
        weigh(i, (5,))
    product(5, 5)
    send("x", [(0, 0)])
    for t, u in ((4, 2), (4, 3), (5, 0), (5, 1), (5, 2), (5, 3), (5, 4)):
        product(t, u)
    wait_sent("y")
    absorb("y", 0)
    wait_sent("x")
    absorb("x", 0)
    wait_sent("z")
    absorb("z", 0)
    absorb("z", 1)
    wait_folds("y")
    unfold("z", 0)
    wait_folds("z")
    unfold("z", 1)


def place_kernel(order, tile, out, sem):
    for r in range(NBLK):
        row = pl.multiple_of(order[0, 0, 0, STORED[r]] * BLK, BLK)
        for c in range(NBLK):
            col = pl.multiple_of(order[0, 0, 0, STORED[c]] * BLK, BLK)
            pltpu.make_async_copy(
                tile.at[r, c], out.at[pl.ds(row, BLK), pl.ds(col, BLK)], sem
            ).start()
    pltpu.make_async_copy(out, out, sem).wait()


def shards(inv_factor, coupling, stiff_gg, block_order):
    full = NBLK * BLK
    hbm = pl.BlockSpec(memory_space=pltpu.HBM)
    smem = pl.BlockSpec(memory_space=pltpu.SMEM)
    vmem = pl.BlockSpec(memory_space=pltpu.VMEM)
    dma = pltpu.SemaphoreType.DMA
    counts = {name: len(NUMBER[name]) for name in "xyz"}
    tile = pl.pallas_call(
        schur_kernel,
        out_shape=pltpu.VMEM((NBLK, NBLK, BLK, BLK), F32),
        in_specs=[hbm, hbm, hbm, hbm],
        out_specs=vmem,
        scratch_shapes=[pltpu.VMEM((NBLK, TILE, BLK), BF16) for _ in range(NTILE)]
        + [pltpu.VMEM((full, full), BF16)]
        + [pltpu.VMEM((NBLK * (NBLK + 1) // 2, BLK, BLK), BF16)]
        + [pltpu.VMEM((full, full), BF16) for _ in range(2)]
        + [pltpu.SMEM((1, 1, 1, NBLK), jnp.int32)]
        + [dma((2 * NTILE + 2,))]
        + [pltpu.VMEM((2, counts[name], BLK, BLK), F32) for name in "xyz"]
        + [dma((2,)) for name in "xyz"]
        + [dma((2, len(BLOCKS[name]))) for name in "xyz"]
        + [pltpu.VMEM((2, len(FOLDS[name]), FOLD, BLK), F32) for name in "yz"]
        + [pltpu.VMEM((2, len(FOLDS[name]), FOLD, BLK), F32) for name in "yz"]
        + [dma((2,)) for name in "yz"]
        + [dma((2, len(FOLDS[name]))) for name in "yz"],
        compiler_params=pltpu.CompilerParams(
            collective_id=0, has_side_effects=True, vmem_limit_bytes=44 << 20
        ),
        name="schur",
    )(
        pltpu.with_memory_space_constraint(block_order, pltpu.HBM),
        inv_factor.reshape(full, full),
        coupling.reshape(full, full),
        stiff_gg.reshape(full, full),
    )
    own = pl.pallas_call(
        place_kernel,
        out_shape=jax.ShapeDtypeStruct((full, full), F32),
        in_specs=[smem, vmem],
        out_specs=hbm,
        scratch_shapes=[dma],
        compiler_params=pltpu.CompilerParams(vmem_limit_bytes=20 << 20),
        name="place",
    )(block_order, tile)
    return own.reshape(1, 1, 1, full, full)


def solution(mesh):
    return jax.shard_map(
        shards,
        mesh=mesh,
        in_specs=(
            P("gx", "gy", "gz", None, None),
            P("gx", "gy", "gz", None, None),
            P("gx", "gy", "gz", None, None),
            P("gx", "gy", "gz", None),
        ),
        out_specs=P("gx", "gy", "gz", None, None),
        check_vma=False,
    )
```

```python
import jax
import jax.numpy as jnp
from jax import lax
from jax.experimental import pallas as pl
from jax.experimental.pallas import tpu as pltpu
from jax.sharding import PartitionSpec as P

BLK = 128
NBLK = 12
TILE = 2 * BLK
NTILE = NBLK // 2
FOLD = BLK + 8
MESH = pl.DeviceIdType.MESH
F32 = jnp.float32
BF16 = jnp.bfloat16

STORED = (8, 9, 10, 11, 4, 6, 5, 7, 2, 3, 0, 1)
PLACE = {block: place for place, block in enumerate(STORED)}

SECTIONS = {
    "x": ("gx", (0,), (1,)),
    "y": ("gy", (8, 10, 2), (9, 11, 3)),
    "z": ("gz", (8, 9, 4, 5), (10, 11, 6, 7)),
}
BLOCKS = {
    "x": (((0, 0),),),
    "y": (((1, 0), (2, 0), (2, 1), (2, 2)),),
    "z": (((1, 0), (2, 0), (2, 1)), ((3, 0), (3, 1), (3, 2))),
}
FOLDS = {"x": (), "y": ((0, 1),), "z": ((2, 3), (0, 1))}
NUMBER = {
    name: {pair: n for n, pair in enumerate(pair for group in groups for pair in group)}
    for name, groups in BLOCKS.items()
}
START = {
    name: [sum(len(group) for group in groups[:g]) for g in range(len(groups))]
    for name, groups in BLOCKS.items()
}


def schur_kernel(order_h, inv_h, cpl_h, stf_h, tile, *scratch):
    scratch = list(scratch)
    cpl = [scratch.pop(0) for _ in range(NTILE)]
    inv, stf, w, wt, order, load_sem = (scratch.pop(0) for _ in range(6))
    got = {name: scratch.pop(0) for name in "xyz"}
    send_sem = {name: scratch.pop(0) for name in "xyz"}
    recv_sem = {name: scratch.pop(0) for name in "xyz"}
    folded = {name: scratch.pop(0) for name in "yz"}
    got_fold = {name: scratch.pop(0) for name in "yz"}
    fold_send_sem = {name: scratch.pop(0) for name in "yz"}
    fold_recv_sem = {name: scratch.pop(0) for name in "yz"}

    def span(i, size=TILE):
        return slice(i * size, (i + 1) * size)

    load_order = pltpu.make_async_copy(order_h, order, load_sem.at[2 * NTILE + 1])
    load_order.start()
    load_inv = []
    for i in range(NTILE):
        area = (span(i), slice(0, (i + 1) * TILE))
        load_inv.append(pltpu.make_async_copy(inv_h.at[area], inv.at[area], load_sem.at[i]))
        load_inv[i].start()
        for s in range(NBLK):
            pltpu.make_async_copy(
                cpl_h.at[span(i), span(s, BLK)], cpl[i].at[s], load_sem.at[NTILE + i]
            ).start()
    for r in range(NBLK):
        for c in range(r + 1):
            pltpu.make_async_copy(
                stf_h.at[span(r, BLK), span(c, BLK)],
                stf.at[r * (r + 1) // 2 + c],
                load_sem.at[2 * NTILE],
            ).start()

    spot = {name: lax.axis_index(SECTIONS[name][0]) for name in "xyz"}
    size = {name: lax.axis_size(SECTIONS[name][0]) for name in "xyz"}
    there = {
        name: (spot[name] > 0, spot[name] < size[name] - 1) for name in "xyz"
    }

    barrier = pltpu.get_barrier_semaphore()
    for name in "xyz":
        for side in (0, 1):

            @pl.when(there[name][side])
            def _(name=name, side=side):
                pl.semaphore_signal(
                    barrier,
                    inc=1,
                    device_id={SECTIONS[name][0]: spot[name] + 2 * side - 1},
                    device_id_type=MESH,
                )

    def greet():
        peers = sum(there[name][side].astype(jnp.int32) for side in (0, 1) for name in "xyz")
        pl.semaphore_wait(barrier, peers)

    def block(a, b):
        return tile.at[PLACE[a], PLACE[b]]

    def remote(name, side, source, target, leave, arrive):
        return pltpu.make_async_remote_copy(
            src_ref=source,
            dst_ref=target,
            send_sem=leave,
            recv_sem=arrive,
            device_id={SECTIONS[name][0]: spot[name] + 2 * side - 1},
            device_id_type=MESH,
        )

    def group_of(name, pair):
        return [pair in group for group in BLOCKS[name]].index(True)

    def clear():
        for name in "xyz":
            for side in (0, 1):

                @pl.when(jnp.logical_not(there[name][side]))
                def _(name=name, side=side):
                    got[name][1 - side] = jnp.zeros(got[name].shape[1:], F32)
                    if FOLDS[name]:
                        got_fold[name][1 - side] = jnp.zeros(got_fold[name].shape[1:], F32)

    def send(name, side, pairs=(), folds=()):
        listed = SECTIONS[name][1 + side]

        @pl.when(there[name][side])
        def _():
            for pair in pairs:
                remote(
                    name,
                    side,
                    block(listed[pair[0]], listed[pair[1]]),
                    got[name].at[side, NUMBER[name][pair]],
                    send_sem[name].at[side],
                    recv_sem[name].at[side, group_of(name, pair)],
                ).start()
            for number in folds:
                remote(
                    name,
                    side,
                    folded[name].at[side, number],
                    got_fold[name].at[side, number],
                    fold_send_sem[name].at[side],
                    fold_recv_sem[name].at[side, number],
                ).start()

    def wait(name, side, sent=False, groups=(), folds=(), folds_sent=False):
        @pl.when(there[name][side])
        def _():
            if sent:
                whole = got[name].at[side]
                remote(
                    name, side, whole, whole, send_sem[name].at[side], recv_sem[name].at[side, 0]
                ).wait_send()
            for group in groups:
                first = START[name][group]
                area = got[name].at[1 - side, slice(first, first + len(BLOCKS[name][group]))]
                remote(
                    name,
                    side,
                    area,
                    area,
                    send_sem[name].at[side],
                    recv_sem[name].at[1 - side, group],
                ).wait_recv()
            for number in folds:
                area = got_fold[name].at[1 - side, number]
                remote(
                    name,
                    side,
                    area,
                    area,
                    fold_send_sem[name].at[side],
                    fold_recv_sem[name].at[1 - side, number],
                ).wait_recv()
            if folds_sent:
                whole = folded[name].at[side]
                remote(
                    name,
                    side,
                    whole,
                    whole,
                    fold_send_sem[name].at[side],
                    fold_recv_sem[name].at[side, 0],
                ).wait_send()

    def absorb(name, group):
        first = START[name][group]
        for side in (0, 1):
            listed = SECTIONS[name][1 + side]
            for n, (i, j) in enumerate(BLOCKS[name][group]):
                a, b = listed[i], listed[j]
                value = block(a, b)[...] + got[name][1 - side, first + n]
                block(a, b)[...] = value
                if i != j:
                    block(b, a)[...] = value.T

    rows = lax.broadcasted_iota(jnp.int32, (BLK, BLK), 0)
    cols = lax.broadcasted_iota(jnp.int32, (BLK, BLK), 1)

    def fold(name, number):
        i, j = FOLDS[name][number]
        for side in (0, 1):
            listed = SECTIONS[name][1 + side]
            one = block(listed[i], listed[i])[...]
            two = block(listed[j], listed[j])[...]
            where = folded[name].at[side, number]
            where[:BLK] = jnp.where(rows >= cols, one, two)
            line = jnp.sum(jnp.where(rows == cols, two, 0.0), axis=0, keepdims=True)
            where[BLK:] = jnp.broadcast_to(line, (FOLD - BLK, BLK))

    def unfold(name, number):
        i, j = FOLDS[name][number]
        for side in (0, 1):
            listed = SECTIONS[name][1 + side]
            area = got_fold[name].at[1 - side, number]
            body = area[:BLK]
            line = area[BLK : BLK + 1]
            flip = body.T
            block(listed[i], listed[i])[...] += jnp.where(rows >= cols, body, flip)
            two = jnp.where(rows == cols, jnp.broadcast_to(line, (BLK, BLK)), flip)
            block(listed[j], listed[j])[...] += jnp.where(rows < cols, body, two)

    def columns(i, tiles):
        return jnp.concatenate(
            [cpl[i][order[0, 0, 0, STORED[s]]] for t in tiles for s in (2 * t, 2 * t + 1)], axis=1
        )

    def weigh(i, tiles):
        depth = (i + 1) * TILE
        right = jnp.concatenate([columns(k, tiles) for k in range(i + 1)], axis=0)
        part = jnp.dot(inv[span(i), :depth], right, preferred_element_type=F32).astype(BF16)
        across = slice(tiles[0] * TILE, (tiles[-1] + 1) * TILE)
        w[span(i), across] = part
        wt[across, span(i)] = part.T

    def stiffness(r, c):
        row, col = order[0, 0, 0, STORED[r]], order[0, 0, 0, STORED[c]]
        high, low = jnp.maximum(row, col), jnp.minimum(row, col)
        held = stf[lax.shift_right_logical(high * (high + 1), 1) + low].astype(F32)
        return held if r == c else jnp.where(row > col, held, held.T)

    later = {
        (lists[side][i], lists[side][j])
        for name, (_, *lists) in SECTIONS.items()
        for pair_groups in BLOCKS[name]
        for i, j in pair_groups
        for side in (0, 1)
        if i != j
    }

    def product(t, u, ready=None):
        both = jnp.dot(wt[span(t), :], w[:, span(u)], preferred_element_type=F32)
        if ready is not None:
            ready()
        for p in range(2):
            for q in range(2):
                r, c = 2 * t + p, 2 * u + q
                if r < c:
                    continue
                value = stiffness(r, c) - both[span(p, BLK), span(q, BLK)]
                tile[r, c] = value
                if r != c and (STORED[r], STORED[c]) not in later:
                    tile[c, r] = value.T

    clear()
    load_order.wait()
    for i in range(NTILE):
        load_inv[i].wait()
        pltpu.make_async_copy(cpl[i], cpl[i], load_sem.at[NTILE + i]).wait()
        weigh(i, (0, 1))

    product(0, 0, pltpu.make_async_copy(stf, stf, load_sem.at[2 * NTILE]).wait)
    product(1, 1)
    product(1, 0)
    fold("y", 0)
    greet()
    for side in (0, 1):
        send("z", side, [(1, 0)])
    for side in (0, 1):
        send("y", side, [(1, 0)], [0])
    for i in range(NTILE):
        weigh(i, (2,))
    product(2, 0)
    product(2, 1)
    for side in (0, 1):
        send("z", side, [(2, 0), (2, 1)])
    product(2, 2)
    for i in range(NTILE):
        weigh(i, (3,))
    product(3, 0)
    product(3, 1)
    product(3, 2)
    product(3, 3)
    fold("z", 0)
    for side in (0, 1):
        send("z", side, [(3, 0), (3, 1), (3, 2)], [0])
    for i in range(NTILE):
        weigh(i, (4,))
    product(4, 0)
    product(4, 1)
    product(4, 4)
    for side in (0, 1):
        send("y", side, [(2, 0), (2, 1), (2, 2)])
    for side in (0, 1):
        wait("y", side, folds=[0])
    unfold("y", 0)
    fold("z", 1)
    for side in (0, 1):
        send("z", side, folds=[1])
    for i in range(NTILE):
        weigh(i, (5,))
    product(5, 5)
    for side in (0, 1):
        send("x", side, [(0, 0)])
    for t, u in ((4, 2), (4, 3), (5, 0), (5, 1), (5, 2), (5, 3), (5, 4)):
        product(t, u)
    for side in (0, 1):
        wait("z", side, sent=True, groups=[0])
    for side in (0, 1):
        wait("x", side, sent=True, groups=[0])
    absorb("z", 0)
    absorb("x", 0)
    for side in (0, 1):
        wait("y", side, sent=True, groups=[0], folds_sent=True)
    absorb("y", 0)
    for side in (0, 1):
        wait("z", side, groups=[1], folds=[0])
    absorb("z", 1)
    unfold("z", 0)
    for side in (0, 1):
        wait("z", side, folds=[1], folds_sent=True)
    unfold("z", 1)


def place_kernel(order, tile, out, sem):
    for r in range(NBLK):
        row = pl.multiple_of(order[0, 0, 0, STORED[r]] * BLK, BLK)
        for c in range(NBLK):
            col = pl.multiple_of(order[0, 0, 0, STORED[c]] * BLK, BLK)
            pltpu.make_async_copy(
                tile.at[r, c], out.at[pl.ds(row, BLK), pl.ds(col, BLK)], sem
            ).start()
    pltpu.make_async_copy(out, out, sem).wait()


def shards(inv_factor, coupling, stiff_gg, block_order):
    full = NBLK * BLK
    hbm = pl.BlockSpec(memory_space=pltpu.HBM)
    smem = pl.BlockSpec(memory_space=pltpu.SMEM)
    vmem = pl.BlockSpec(memory_space=pltpu.VMEM)
    dma = pltpu.SemaphoreType.DMA
    counts = {name: len(NUMBER[name]) for name in "xyz"}
    tile = pl.pallas_call(
        schur_kernel,
        out_shape=pltpu.VMEM((NBLK, NBLK, BLK, BLK), F32),
        in_specs=[hbm, hbm, hbm, hbm],
        out_specs=vmem,
        scratch_shapes=[pltpu.VMEM((NBLK, TILE, BLK), BF16) for _ in range(NTILE)]
        + [pltpu.VMEM((full, full), BF16)]
        + [pltpu.VMEM((NBLK * (NBLK + 1) // 2, BLK, BLK), BF16)]
        + [pltpu.VMEM((full, full), BF16) for _ in range(2)]
        + [pltpu.SMEM((1, 1, 1, NBLK), jnp.int32)]
        + [dma((2 * NTILE + 2,))]
        + [pltpu.VMEM((2, counts[name], BLK, BLK), F32) for name in "xyz"]
        + [dma((2,)) for name in "xyz"]
        + [dma((2, len(BLOCKS[name]))) for name in "xyz"]
        + [pltpu.VMEM((2, len(FOLDS[name]), FOLD, BLK), F32) for name in "yz"]
        + [pltpu.VMEM((2, len(FOLDS[name]), FOLD, BLK), F32) for name in "yz"]
        + [dma((2,)) for name in "yz"]
        + [dma((2, len(FOLDS[name]))) for name in "yz"],
        compiler_params=pltpu.CompilerParams(
            collective_id=0, has_side_effects=True, vmem_limit_bytes=44 << 20
        ),
        name="schur",
    )(
        pltpu.with_memory_space_constraint(block_order, pltpu.HBM),
        inv_factor.reshape(full, full),
        coupling.reshape(full, full),
        stiff_gg.reshape(full, full),
    )
    own = pl.pallas_call(
        place_kernel,
        out_shape=jax.ShapeDtypeStruct((full, full), F32),
        in_specs=[smem, vmem],
        out_specs=hbm,
        scratch_shapes=[dma],
        compiler_params=pltpu.CompilerParams(vmem_limit_bytes=20 << 20),
        name="place",
    )(block_order, tile)
    return own.reshape(1, 1, 1, full, full)


def solution(mesh):
    return jax.shard_map(
        shards,
        mesh=mesh,
        in_specs=(
            P("gx", "gy", "gz", None, None),
            P("gx", "gy", "gz", None, None),
            P("gx", "gy", "gz", None, None),
            P("gx", "gy", "gz", None),
        ),
        out_specs=P("gx", "gy", "gz", None, None),
        check_vma=False,
    )
```

```python
import jax
import jax.numpy as jnp
from jax import lax
from jax.experimental import pallas as pl
from jax.experimental.pallas import tpu as pltpu
from jax.sharding import PartitionSpec as P

BLK = 128
NBLK = 12
TILE = 2 * BLK
NTILE = NBLK // 2
FOLD = BLK + 8
MESH = pl.DeviceIdType.MESH
F32 = jnp.float32
BF16 = jnp.bfloat16

STORED = (8, 9, 10, 11, 4, 6, 5, 7, 2, 3, 0, 1)
PLACE = {block: place for place, block in enumerate(STORED)}

SECTIONS = {
    "x": ("gx", (0,), (1,)),
    "y": ("gy", (8, 10, 2), (9, 11, 3)),
    "z": ("gz", (8, 9, 4, 5), (10, 11, 6, 7)),
}
BLOCKS = {
    "x": (((0, 0),),),
    "y": (((1, 0), (2, 0), (2, 1), (2, 2)),),
    "z": (((1, 0),), ((2, 0), (2, 1),), ((3, 1),), ((3, 0), (3, 2),), ),
}
RELAYED = 2
FOLDS = {"x": (), "y": ((0, 1),), "z": ((2, 3), (0, 1))}
NUMBER = {
    name: {pair: n for n, pair in enumerate(pair for group in groups for pair in group)}
    for name, groups in BLOCKS.items()
}
START = {
    name: [sum(len(group) for group in groups[:g]) for g in range(len(groups))]
    for name, groups in BLOCKS.items()
}


def schur_kernel(order_h, inv_h, cpl_h, stf_h, tile, *scratch):
    scratch = list(scratch)
    cpl = [scratch.pop(0) for _ in range(NTILE)]
    inv, stf, w, wt, order, load_sem = (scratch.pop(0) for _ in range(6))
    got = {name: scratch.pop(0) for name in "xyz"}
    send_sem = {name: scratch.pop(0) for name in "xyz"}
    recv_sem = {name: scratch.pop(0) for name in "xyz"}
    folded = {name: scratch.pop(0) for name in "yz"}
    got_fold = {name: scratch.pop(0) for name in "yz"}
    fold_send_sem = {name: scratch.pop(0) for name in "yz"}
    fold_recv_sem = {name: scratch.pop(0) for name in "yz"}

    def span(i, size=TILE):
        return slice(i * size, (i + 1) * size)

    load_order = pltpu.make_async_copy(order_h, order, load_sem.at[2 * NTILE + 1])
    load_order.start()
    load_inv = []
    for i in range(NTILE):
        area = (span(i), slice(0, (i + 1) * TILE))
        load_inv.append(pltpu.make_async_copy(inv_h.at[area], inv.at[area], load_sem.at[i]))
        load_inv[i].start()
        for s in range(NBLK):
            pltpu.make_async_copy(
                cpl_h.at[span(i), span(s, BLK)], cpl[i].at[s], load_sem.at[NTILE + i]
            ).start()
    for r in range(NBLK):
        for c in range(r + 1):
            pltpu.make_async_copy(
                stf_h.at[span(r, BLK), span(c, BLK)],
                stf.at[r * (r + 1) // 2 + c],
                load_sem.at[2 * NTILE],
            ).start()

    spot = {name: lax.axis_index(SECTIONS[name][0]) for name in "xyz"}
    size = {name: lax.axis_size(SECTIONS[name][0]) for name in "xyz"}
    there = {
        name: (spot[name] > 0, spot[name] < size[name] - 1) for name in "xyz"
    }

    half = size["z"] // 2
    at = {place: spot["z"] == place for place in (0, half - 1, half)}

    def aim(name, side, relayed=False):
        target = spot[name] + 2 * side - 1
        if relayed:
            target = jnp.where(at[half - 1], 0, target)
        return {SECTIONS[name][0]: target}

    barrier = pltpu.get_barrier_semaphore()
    for name in "xyz":
        for side in (0, 1):

            @pl.when(there[name][side])
            def _(name=name, side=side):
                pl.semaphore_signal(
                    barrier,
                    inc=1,
                    device_id={SECTIONS[name][0]: spot[name] + 2 * side - 1},
                    device_id_type=MESH,
                )

    for one, two in ((half - 1, 0), (0, half - 1), (0, half), (half, 0)):

        @pl.when(at[one])
        def _(two=two):
            pl.semaphore_signal(
                barrier, inc=1, device_id={"gz": jnp.int32(two)}, device_id_type=MESH
            )

    def greet():
        peers = sum(there[name][side].astype(jnp.int32) for side in (0, 1) for name in "xyz")
        for one in (half - 1, 0, 0, half):
            peers += at[one].astype(jnp.int32)
        pl.semaphore_wait(barrier, peers)

    def block(a, b):
        return tile.at[PLACE[a], PLACE[b]]

    def remote(name, side, source, target, leave, arrive, relayed=False):
        return pltpu.make_async_remote_copy(
            src_ref=source,
            dst_ref=target,
            send_sem=leave,
            recv_sem=arrive,
            device_id=aim(name, side, relayed),
            device_id_type=MESH,
        )

    def group_of(name, pair):
        return [pair in group for group in BLOCKS[name]].index(True)

    def clear():
        for name in "xyz":
            for side in (0, 1):

                @pl.when(jnp.logical_not(there[name][side]))
                def _(name=name, side=side):
                    if name != "z" or side != 0:
                        got[name][1 - side] = jnp.zeros(got[name].shape[1:], F32)
                    if FOLDS[name]:
                        got_fold[name][1 - side] = jnp.zeros(got_fold[name].shape[1:], F32)

    def send(name, side, pairs=(), folds=()):
        listed = SECTIONS[name][1 + side]

        @pl.when(there[name][side])
        def _():
            for pair in pairs:
                remote(
                    name,
                    side,
                    block(listed[pair[0]], listed[pair[1]]),
                    got[name].at[side, NUMBER[name][pair]],
                    send_sem[name].at[side],
                    recv_sem[name].at[side, group_of(name, pair)],
                    name == "z" and side == 1 and group_of(name, pair) < RELAYED,
                ).start()
            for number in folds:
                remote(
                    name,
                    side,
                    folded[name].at[side, number],
                    got_fold[name].at[side, number],
                    fold_send_sem[name].at[side],
                    fold_recv_sem[name].at[side, number],
                ).start()

    def passing(group, whole=False):
        first, last = START["z"][group], START["z"][group] + len(BLOCKS["z"][group])
        if whole:
            last = START["z"][RELAYED - 1] + len(BLOCKS["z"][RELAYED - 1])
        area = got["z"].at[1, slice(first, last)]
        return pltpu.make_async_remote_copy(
            src_ref=area,
            dst_ref=area,
            send_sem=send_sem["z"].at[0],
            recv_sem=recv_sem["z"].at[1, group],
            device_id={"gz": jnp.int32(half)},
            device_id_type=MESH,
        )

    def pass_on(groups):
        @pl.when(at[0])
        def _():
            for group in groups:
                copy = passing(group)
                copy.wait_recv()
                copy.start()

    def wait_passed():
        @pl.when(at[0])
        def _():
            passing(0, True).wait_send()
            got["z"][1] = jnp.zeros(got["z"].shape[1:], F32)

    def wait(name, side, sent=False, groups=(), folds=(), folds_sent=False):
        @pl.when(there[name][side])
        def _():
            if sent:
                whole = got[name].at[side]
                remote(
                    name, side, whole, whole, send_sem[name].at[side], recv_sem[name].at[side, 0]
                ).wait_send()
            for group in groups:
                first = START[name][group]
                area = got[name].at[1 - side, slice(first, first + len(BLOCKS[name][group]))]
                remote(
                    name,
                    side,
                    area,
                    area,
                    send_sem[name].at[side],
                    recv_sem[name].at[1 - side, group],
                ).wait_recv()
            for number in folds:
                area = got_fold[name].at[1 - side, number]
                remote(
                    name,
                    side,
                    area,
                    area,
                    fold_send_sem[name].at[side],
                    fold_recv_sem[name].at[1 - side, number],
                ).wait_recv()
            if folds_sent:
                whole = folded[name].at[side]
                remote(
                    name,
                    side,
                    whole,
                    whole,
                    fold_send_sem[name].at[side],
                    fold_recv_sem[name].at[side, 0],
                ).wait_send()

    def absorb(name, group):
        first = START[name][group]
        for side in (0, 1):
            listed = SECTIONS[name][1 + side]
            for n, (i, j) in enumerate(BLOCKS[name][group]):
                a, b = listed[i], listed[j]
                value = block(a, b)[...] + got[name][1 - side, first + n]
                block(a, b)[...] = value
                if i != j:
                    block(b, a)[...] = value.T

    rows = lax.broadcasted_iota(jnp.int32, (BLK, BLK), 0)
    cols = lax.broadcasted_iota(jnp.int32, (BLK, BLK), 1)

    def fold(name, number):
        i, j = FOLDS[name][number]
        for side in (0, 1):
            listed = SECTIONS[name][1 + side]
            one = block(listed[i], listed[i])[...]
            two = block(listed[j], listed[j])[...]
            where = folded[name].at[side, number]
            where[:BLK] = jnp.where(rows >= cols, one, two)
            line = jnp.sum(jnp.where(rows == cols, two, 0.0), axis=0, keepdims=True)
            where[BLK:] = jnp.broadcast_to(line, (FOLD - BLK, BLK))

    def unfold(name, number):
        i, j = FOLDS[name][number]
        for side in (0, 1):
            listed = SECTIONS[name][1 + side]
            area = got_fold[name].at[1 - side, number]
            body = area[:BLK]
            line = area[BLK : BLK + 1]
            flip = body.T
            block(listed[i], listed[i])[...] += jnp.where(rows >= cols, body, flip)
            two = jnp.where(rows == cols, jnp.broadcast_to(line, (BLK, BLK)), flip)
            block(listed[j], listed[j])[...] += jnp.where(rows < cols, body, two)

    def columns(i, tiles):
        return jnp.concatenate(
            [cpl[i][order[0, 0, 0, STORED[s]]] for t in tiles for s in (2 * t, 2 * t + 1)], axis=1
        )

    def weigh(i, tiles):
        depth = (i + 1) * TILE
        right = jnp.concatenate([columns(k, tiles) for k in range(i + 1)], axis=0)
        part = jnp.dot(inv[span(i), :depth], right, preferred_element_type=F32).astype(BF16)
        across = slice(tiles[0] * TILE, (tiles[-1] + 1) * TILE)
        w[span(i), across] = part
        wt[across, span(i)] = part.T

    def stiffness(r, c):
        row, col = order[0, 0, 0, STORED[r]], order[0, 0, 0, STORED[c]]
        high, low = jnp.maximum(row, col), jnp.minimum(row, col)
        held = stf[lax.shift_right_logical(high * (high + 1), 1) + low].astype(F32)
        return held if r == c else jnp.where(row > col, held, held.T)

    later = {
        (lists[side][i], lists[side][j])
        for name, (_, *lists) in SECTIONS.items()
        for pair_groups in BLOCKS[name]
        for i, j in pair_groups
        for side in (0, 1)
        if i != j
    }

    def product(t, u, ready=None):
        both = jnp.dot(wt[span(t), :], w[:, span(u)], preferred_element_type=F32)
        if ready is not None:
            ready()
        for p in range(2):
            for q in range(2):
                r, c = 2 * t + p, 2 * u + q
                if r < c:
                    continue
                value = stiffness(r, c) - both[span(p, BLK), span(q, BLK)]
                tile[r, c] = value
                if r != c and (STORED[r], STORED[c]) not in later:
                    tile[c, r] = value.T

    clear()
    load_order.wait()
    for i in range(NTILE):
        load_inv[i].wait()
        pltpu.make_async_copy(cpl[i], cpl[i], load_sem.at[NTILE + i]).wait()
        weigh(i, (0, 1))

    product(0, 0, pltpu.make_async_copy(stf, stf, load_sem.at[2 * NTILE]).wait)
    greet()
    send("z", 0, [(1, 0)])
    product(1, 1)
    product(1, 0)
    fold("y", 0)
    send("z", 1, [(1, 0)])
    for side in (0, 1):
        send("y", side, [(1, 0)], [0])
    for i in range(NTILE):
        weigh(i, (2,))
    product(2, 0)
    product(2, 1)
    for side in (0, 1):
        send("z", side, [(2, 0), (2, 1)])
    for i in range(NTILE):
        weigh(i, (3,))
    product(3, 0)
    product(3, 1)
    product(3, 2)
    for side in (1, 0):
        send("z", side, [(3, 0), (3, 1), (3, 2)])
    product(2, 2)
    product(3, 3)
    fold("z", 0)
    for side in (1, 0):
        send("z", side, folds=[0])
    for i in range(NTILE):
        weigh(i, (4,))
    product(4, 0)
    product(4, 1)
    product(4, 4)
    for side in (0, 1):
        send("y", side, [(2, 0), (2, 1), (2, 2)])
    for side in (0, 1):
        wait("y", side, folds=[0])
    unfold("y", 0)
    fold("z", 1)
    for side in (0, 1):
        send("z", side, folds=[1])
    for i in range(NTILE):
        weigh(i, (5,))
    product(5, 5)
    for side in (0, 1):
        send("x", side, [(0, 0)])
    for t, u in ((4, 2), (4, 3), (5, 0)):
        product(t, u)
    pass_on([0])
    for t, u in ((5, 1), (5, 2), (5, 3), (5, 4)):
        product(t, u)
    pass_on([1])
    for side in (0, 1):
        wait("x", side, sent=True, groups=[0])
    absorb("x", 0)
    for side in (0, 1):
        wait("y", side, sent=True, groups=[0], folds_sent=True)
    absorb("y", 0)
    wait_passed()
    for side in (0, 1):
        wait("z", side, sent=True, groups=[0, 1])
    absorb("z", 0)
    absorb("z", 1)
    for side in (0, 1):
        wait("z", side, groups=[3], folds=[0])
    absorb("z", 3)
    unfold("z", 0)
    for side in (0, 1):
        wait("z", side, groups=[2], folds=[1], folds_sent=True)
    absorb("z", 2)
    unfold("z", 1)


def place_kernel(order, tile, out, sem):
    for r in range(NBLK):
        row = pl.multiple_of(order[0, 0, 0, STORED[r]] * BLK, BLK)
        for c in range(NBLK):
            col = pl.multiple_of(order[0, 0, 0, STORED[c]] * BLK, BLK)
            pltpu.make_async_copy(
                tile.at[r, c], out.at[pl.ds(row, BLK), pl.ds(col, BLK)], sem
            ).start()
    pltpu.make_async_copy(out, out, sem).wait()


def shards(inv_factor, coupling, stiff_gg, block_order):
    full = NBLK * BLK
    hbm = pl.BlockSpec(memory_space=pltpu.HBM)
    smem = pl.BlockSpec(memory_space=pltpu.SMEM)
    vmem = pl.BlockSpec(memory_space=pltpu.VMEM)
    dma = pltpu.SemaphoreType.DMA
    counts = {name: len(NUMBER[name]) for name in "xyz"}
    tile = pl.pallas_call(
        schur_kernel,
        out_shape=pltpu.VMEM((NBLK, NBLK, BLK, BLK), F32),
        in_specs=[hbm, hbm, hbm, hbm],
        out_specs=vmem,
        scratch_shapes=[pltpu.VMEM((NBLK, TILE, BLK), BF16) for _ in range(NTILE)]
        + [pltpu.VMEM((full, full), BF16)]
        + [pltpu.VMEM((NBLK * (NBLK + 1) // 2, BLK, BLK), BF16)]
        + [pltpu.VMEM((full, full), BF16) for _ in range(2)]
        + [pltpu.SMEM((1, 1, 1, NBLK), jnp.int32)]
        + [dma((2 * NTILE + 2,))]
        + [pltpu.VMEM((2, counts[name], BLK, BLK), F32) for name in "xyz"]
        + [dma((2,)) for name in "xyz"]
        + [dma((2, len(BLOCKS[name]))) for name in "xyz"]
        + [pltpu.VMEM((2, len(FOLDS[name]), FOLD, BLK), F32) for name in "yz"]
        + [pltpu.VMEM((2, len(FOLDS[name]), FOLD, BLK), F32) for name in "yz"]
        + [dma((2,)) for name in "yz"]
        + [dma((2, len(FOLDS[name]))) for name in "yz"],
        compiler_params=pltpu.CompilerParams(
            collective_id=0, has_side_effects=True, vmem_limit_bytes=44 << 20
        ),
        name="schur",
    )(
        pltpu.with_memory_space_constraint(block_order, pltpu.HBM),
        inv_factor.reshape(full, full),
        coupling.reshape(full, full),
        stiff_gg.reshape(full, full),
    )
    own = pl.pallas_call(
        place_kernel,
        out_shape=jax.ShapeDtypeStruct((full, full), F32),
        in_specs=[smem, vmem],
        out_specs=hbm,
        scratch_shapes=[dma],
        compiler_params=pltpu.CompilerParams(vmem_limit_bytes=20 << 20),
        name="place",
    )(block_order, tile)
    return own.reshape(1, 1, 1, full, full)


def solution(mesh):
    return jax.shard_map(
        shards,
        mesh=mesh,
        in_specs=(
            P("gx", "gy", "gz", None, None),
            P("gx", "gy", "gz", None, None),
            P("gx", "gy", "gz", None, None),
            P("gx", "gy", "gz", None),
        ),
        out_specs=P("gx", "gy", "gz", None, None),
        check_vma=False,
    )
```
